32 devices in a mesh: row: 8 (over z, y), col: 4 (over x, core).
Axes of the slice: x: 2, y: 2, z: 4, core: 2. Of those that a mesh axis runs over, the one named last changes fastest.
Arguments:
- coeffs: bfloat16 [4096, 1024], P(('row', 'col')), may hold values from -0.1875 to 0.1875
- h_blocks: bfloat16 [8, 4, 8, 4, 128, 128], P('row', 'col'), may hold values from -18 to 18
- block_codes: int32 [8, 4, 8, 4], P('row', 'col'), may hold values from 0 to 4, as said below
Outputs:
- gram: float32 [1024, 1024], P('row', 'col')
The draws below stay inside these ranges and needn't reach their ends.
Inputs may be any that keep to these rules, and one draw needn't show every extreme that they name: The value 4 * 1 marks an empty slot; the other values within one sub-panel block_codes[r, c, p, :] are distinct. Every tile [r, c] has a sub-panel with no empty slot.
All inputs are finite; a program needn't handle non-finite values.
Results may differ from the reference program's by a relative error of at most 0.0003.
Values may be sent and summed in bfloat16 or wider, within the bound.
A program may use at most 128 MiB of HBM per device.

```python
import jax
import jax.numpy as jnp
from jax import lax

BLK = 128
ORBITALS = 1024
CAP = 4
ORDER = 4096
PANEL_BLOCKS = 1
TILE_BROWS = 4
N_ROW = 8
N_COL = 4


def draw_block_codes(key, part):
    slot_count = TILE_BROWS * PANEL_BLOCKS
    panels = N_ROW * N_COL * N_ROW
    key_order, key_count, key_full = jax.random.split(jax.random.fold_in(key, 11), 3)
    scores = jax.random.randint(key_order, (panels, slot_count), 0, 1 << 20) * slot_count + jnp.arange(slot_count, dtype=jnp.int32)[None, :]
    ranked = jnp.argsort(scores, axis=1)[:, :CAP].astype(jnp.int32)
    counts = jax.random.randint(key_count, (N_ROW * N_COL, N_ROW), 2, CAP + 1)
    full_index = jax.random.randint(key_full, (N_ROW * N_COL, 1), 0, N_ROW)
    counts = jnp.where(jnp.arange(N_ROW)[None, :] == full_index, CAP, counts).reshape(panels, 1)
    is_live = jnp.arange(CAP)[None, :] < counts
    codes_all = jnp.where(is_live, ranked, slot_count)
    return codes_all.reshape(N_ROW, N_COL, N_ROW, CAP).astype(jnp.int32)


def strengthened(entries, stream_key, source, target, blocks, factor):
    owner, partner = [(jnp.arange(entries.shape[dim]) // (entries.shape[dim] // blocks)).reshape([-1 if axis == dim else 1 for axis in range(entries.ndim)]) for dim in (source, target)]
    chosen = jax.random.permutation(stream_key, blocks)[partner]
    strong = (owner == chosen) | (owner == (partner + blocks // 2) % blocks)
    return jnp.where(strong, factor * entries, entries)


def block_scale(rng, extent, pieces, least, largest):
    gain, own = 1.0, jax.random.fold_in(rng, 6)
    for dim, parts in pieces:
        heights = jnp.exp(jax.random.uniform(jax.random.fold_in(own, dim), (parts,), jnp.float32, least / len(pieces), largest / len(pieces)))
        gain = gain * jnp.repeat(heights, extent[dim] // parts).reshape([-1 if axis == dim else 1 for axis in range(len(extent))])
    return gain


def normal_values(stream_key, extent, scale, limit, shards=(), held_as=jnp.bfloat16):
    array = jax.random.normal(stream_key, extent, jnp.float32) * scale
    if len(shards) > 0:
        array = block_scale(stream_key, extent, shards, -0.22, 0.18) * array
    return jnp.clip(array, min=-limit, max=limit).astype(held_as)


def bell_draw_with(own_key, shape, width, most, cuts, heavy, kind=jnp.bfloat16):
    drawn = width * jax.random.normal(own_key, shape, jnp.float32)
    if cuts:
        drawn = drawn * block_scale(own_key, shape, cuts, -0.22, 0.18)
    return jnp.clip(strengthened(drawn, jax.random.fold_in(own_key, 3), *heavy), -most, most).astype(kind)


def setup_inputs(seed: int = 0) -> dict:
    streams_of = jax.random.split(jax.random.key(seed), 4)
    return {
        "coeffs": bell_draw_with(streams_of[0], (ORDER, ORBITALS), ORDER ** -0.5, 0.1875, ((0, 32),), (0, 1, 32, 2.75)),
        "h_blocks": normal_values(streams_of[1], (N_ROW, N_COL, N_ROW, CAP, BLK, BLK), 3.0, 18.0, ((0, 8), (1, 4))),
        "block_codes": draw_block_codes(jax.random.fold_in(streams_of[3], 71), 0),
    }


def tile_product(coeffs, h_blocks, block_codes, row_index):
    orbital_width = coeffs.shape[1]
    empty_code = TILE_BROWS * PANEL_BLOCKS
    panel_data = coeffs.reshape(N_ROW, N_COL, PANEL_BLOCKS, BLK, orbital_width).transpose(1, 0, 2, 3, 4)
    row_blocks = lax.dynamic_index_in_dim(h_blocks, row_index, 0, keepdims=False)
    row_codes = lax.dynamic_index_in_dim(block_codes, row_index, 0, keepdims=False)

    def add_tile(running, inputs):
        blocks, codes, panel = inputs
        is_live = (codes < empty_code).astype(jnp.float32)
        block_row = jnp.minimum(codes // PANEL_BLOCKS, TILE_BROWS - 1).astype(jnp.int32)
        within = (codes % PANEL_BLOCKS).astype(jnp.int32)
        selector = (within[:, :, None] == jnp.arange(PANEL_BLOCKS, dtype=jnp.int32)[None, None, :]).astype(jnp.float32)
        chosen = jnp.einsum("psq,pqjk->psjk", selector, panel.astype(jnp.float32))
        product = jnp.einsum("psij,psjk->psik", blocks.astype(jnp.float32), chosen) * is_live[:, :, None, None]
        running = running.at[block_row.reshape(-1)].add(product.reshape(-1, BLK, orbital_width))
        return running, None

    zero_rows = jnp.zeros((TILE_BROWS, BLK, orbital_width), jnp.float32)
    result, unused = lax.scan(add_tile, zero_rows, (row_blocks, row_codes, panel_data))
    return result.reshape(TILE_BROWS * BLK, orbital_width)


def reference(coeffs, h_blocks, block_codes):
    orbital_width = coeffs.shape[1]
    group_rows = TILE_BROWS * BLK

    def add_group(gram, row_index):
        applied = tile_product(coeffs, h_blocks, block_codes, row_index)
        left_rows = lax.dynamic_slice_in_dim(coeffs, row_index * group_rows, group_rows, 0).astype(jnp.float32)
        gram = gram + jnp.dot(left_rows.T, applied, precision=lax.Precision.HIGHEST)
        return gram, None

    start_gram = jnp.zeros((orbital_width, orbital_width), jnp.float32)
    gram, unused = lax.scan(add_group, start_gram, jnp.arange(N_ROW, dtype=jnp.int32))
    return gram
```

```python
import functools

import jax
import jax.numpy as jnp
from jax import lax
from jax.experimental import pallas as pl
from jax.experimental.pallas import tpu as pltpu
from jax.sharding import PartitionSpec as P

BLK = 128
CAP = 4
MESH = pl.DeviceIdType.MESH


def ring_order(mesh):
    rows = mesh.shape["row"]
    devices = mesh.devices.reshape(rows, -1)[:, 0]
    try:
        spots = [tuple(int(v) for v in d.coords) for d in devices]
    except (AttributeError, TypeError):
        return list(range(rows))
    axes = [a for a in range(len(spots[0])) if len({s[a] for s in spots}) > 1]
    if len(axes) != 2 or len(set(spots)) != rows:
        return list(range(rows))
    index = {(s[axes[0]], s[axes[1]]): i for i, s in enumerate(spots)}
    first = sorted({s[axes[0]] for s in spots})
    second = sorted({s[axes[1]] for s in spots})
    if len(first) % 2:
        return list(range(rows))
    cycle = []
    for n, a in enumerate(first):
        inner = second[1:] if n % 2 == 0 else second[:0:-1]
        cycle += [(a, b) for b in inner]
    cycle += [(a, second[0]) for a in reversed(first)]
    return [index[key] for key in cycle]


def kernel(order, rc, cc, coeffs, blocks, codes, out,
           cr, hall, codes_all, g, acc, dense, gram, rin,
           local_sem, dir_send, dir_recv, par_send, par_recv,
           own_send, own_recv, ring_send, ring_recv, rs_send, rs_recv):
    r = lax.axis_index("row")
    c = lax.axis_index("col")
    x, k = c // 2, c % 2
    nx = cc // 2
    partner = c + 1 - 2 * k
    half = rc // 2
    width = out.shape[1]
    tall = out.shape[0]
    part = tall // 2
    tb = dense.shape[0] // BLK

    def look(table, i):
        value = jnp.int32(table[0])
        for n in range(1, len(table)):
            value = jnp.where(i == n, jnp.int32(table[n]), value)
        return value

    place = [0] * rc
    for n, row in enumerate(order):
        place[row] = n
    pos = look(place, r)
    behind = [r] + [look(order, lax.rem(pos + rc - s, rc)) for s in range(1, rc)]
    left, right = behind[1], behind[rc - 1]

    def xcol(d, kk):
        return lax.rem(x + nx - d, nx) * 2 + kk

    def cols(i, w):
        return pl.ds(pl.multiple_of(i * w, w), w)

    barrier = pltpu.get_barrier_semaphore()
    friends = [(left, c), (right, c), (r, partner)]
    friends += [(r, xcol(d, k)) for d in range(1, nx)]
    for friend in friends:
        pl.semaphore_signal(barrier, inc=1, device_id=friend, device_id_type=MESH)
    pl.semaphore_wait(barrier, len(friends))

    sent = []

    def send(src, dst, ssem, rsem, device):
        copy = pltpu.make_async_remote_copy(
            src_ref=src, dst_ref=dst, send_sem=ssem, recv_sem=rsem,
            device_id=device, device_id_type=MESH)
        copy.start()
        sent.append(copy)

    def arrived(dst, ssem, rsem, device):
        pltpu.make_async_remote_copy(
            src_ref=dst, dst_ref=dst, send_sem=ssem, recv_sem=rsem,
            device_id=device, device_id_type=MESH).wait_recv()

    def item_ref(source, base_x, n):
        if n < nx:
            return cr.at[source, :, cols(lax.rem(base_x + n, nx), 2 * width)]
        if n == nx:
            return codes_all.at[source]
        return hall.at[source, behind[n - nx - 1]]

    def item_src(base_x, n):
        if n < nx:
            return coeffs.at[:, cols(lax.rem(base_x + n, nx), 2 * width)]
        if n == nx:
            return codes
        return blocks.at[behind[n - nx - 1]]

    def send_item(d, n):
        tx = lax.rem(x + d, nx)
        send(item_src(tx, n), item_ref(c, tx, n), dir_send.at[d - 1, n],
             dir_recv.at[d - 1, n], (r, tx * 2 + k))

    def relay_item(d, n):
        src = item_ref(xcol(d, k), x, n)
        arrived(src, dir_send.at[d - 1, n], dir_recv.at[d - 1, n], (r, xcol(d, k)))
        send(src, src, par_send.at[d - 1, n], par_recv.at[d - 1, n], (r, partner))

    def take_item(d, n):
        dst = item_ref(xcol(d, 1 - k), x, n)
        arrived(dst, par_send.at[d - 1, n], par_recv.at[d - 1, n], (r, partner))

    def moves(step, j, way):
        if step < 1 or step > half:
            return False
        if step == half and rc % 2 == 0:
            return (j % 2) == way
        return True

    def slot(step, way):
        return step if way == 0 else rc - step

    def chunk_col(j):
        return xcol(j // 2, k if j % 2 == 0 else 1 - k)

    def ring_send_to(src, step, j, way):
        send(src, g.at[slot(step, way), chunk_col(j)], ring_send.at[way, step - 1, j],
             ring_recv.at[way, step - 1, j], (right if way == 0 else left, c))

    def ring_first(src, j):
        for way in range(2):
            if moves(1, j, way):
                ring_send_to(src, 1, j, way)

    copies = [
        pltpu.make_async_copy(coeffs, cr.at[c], local_sem.at[0]),
        pltpu.make_async_copy(blocks, hall.at[c], local_sem.at[1]),
        pltpu.make_async_copy(codes, codes_all.at[c], local_sem.at[2]),
    ]
    ring_first(coeffs.at[:, cols(c, width)], 0)
    for d in range(1, nx):
        send_item(d, 0)
    own = [(coeffs, cr.at[c], cr.at[partner]), (codes, codes_all.at[c], codes_all.at[partner]),
           (blocks, hall.at[c], hall.at[partner])]
    for n, (src, dst, _) in enumerate(own):
        send(src, dst, own_send.at[n], own_recv.at[n], (r, partner))
    for copy in copies:
        copy.start()
    hblock = nx + 1
    last_block = hblock + half
    for d in range(1, nx):
        send_item(d, nx)
    sequence = [0]
    for s in range(1, half):
        sequence += [s, rc - s]
    for s in sequence:
        for d in range(1, nx):
            send_item(d, hblock + s)
    for n in range(1, nx):
        for d in range(1, nx):
            send_item(d, n)
    for d in range(1, nx):
        send_item(d, last_block)

    def own_arrived(n):
        arrived(own[n][2], own_send.at[n], own_recv.at[n], (r, partner))

    own_arrived(0)
    ring_first(cr.at[partner, :, cols(c, width)], 1)
    for d in range(1, nx):
        relay_item(d, 0)
        ring_first(cr.at[xcol(d, k), :, cols(c, width)], 2 * d)
        take_item(d, 0)
        ring_first(cr.at[xcol(d, 1 - k), :, cols(c, width)], 2 * d + 1)
    for d in range(1, nx):
        relay_item(d, nx)
    for copy in copies:
        copy.wait()
    own_arrived(1)
    own_arrived(2)
    for d in range(1, nx):
        take_item(d, nx)

    acc[...] = jnp.zeros_like(acc)

    def accumulate(s, xx):
        p = behind[s]
        for kk in range(2):
            tile = xx * 2 + kk
            code = codes_all[tile, pl.ds(p, 1), :]
            block = [hall[tile, p, t] for t in range(CAP)]
            for b in range(tb):
                hit = jnp.where(code == b, 1.0, 0.0).astype(jnp.float32)
                total = None
                for t in range(CAP):
                    pick = jnp.broadcast_to(hit[:, t:t + 1], (1, BLK)).astype(jnp.bfloat16)
                    term = block[t] * pick
                    total = term if total is None else total + term
                dense[pl.ds(b * BLK, BLK), pl.ds(kk * BLK, BLK)] = total
        if s == 0:
            rows = cr[pl.ds(xx * 2, 2), :, cols(c, width)]
        else:
            rows = g[s, pl.ds(xx * 2, 2)]
        acc[...] += jnp.dot(dense[...], rows.reshape(2 * BLK, width),
                            preferred_element_type=jnp.float32)

    def at_distance(s):
        if s == 0 or (2 * s == rc):
            return [s]
        return [s, rc - s]

    accumulate(0, x)
    for step in range(1, half + 1):
        for j in range(cc):
            for way in range(2):
                if moves(step, j, way):
                    here = g.at[slot(step, way), chunk_col(j)]
                    arrived(here, ring_send.at[way, step - 1, j],
                            ring_recv.at[way, step - 1, j],
                            (left if way == 0 else right, c))
                    if moves(step + 1, j, way):
                        ring_send_to(here, step + 1, j, way)
        for s in at_distance(step - 1):
            for d in range(1, nx):
                relay_item(d, hblock + s)
        for s in at_distance(step):
            accumulate(s, x)
        for s in at_distance(step - 1):
            for d in range(1, nx):
                take_item(d, hblock + s)
                accumulate(s, lax.rem(x + nx - d, nx))
    for n in range(1, nx):
        for d in range(1, nx):
            relay_item(d, n)
    for n in range(1, nx):
        for d in range(1, nx):
            take_item(d, n)
    for d in range(1, nx):
        relay_item(d, last_block)
    for d in range(1, nx):
        take_item(d, last_block)
        accumulate(half, lax.rem(x + nx - d, nx))

    applied = acc[...]
    high = applied.astype(jnp.bfloat16)
    low = (applied - high.astype(jnp.float32)).astype(jnp.bfloat16)
    contract = (((0,), (0,)), ((), ()))
    orbitals = coeffs.shape[1]
    step_cols = min(256, orbitals)
    for i in range(orbitals // step_cols):
        lhs = cr[:, :, pl.ds(i * step_cols, step_cols)].reshape(cc * coeffs.shape[0], step_cols)
        gram[pl.ds(i * step_cols, step_cols), :] = (
            lax.dot_general(lhs, high, contract, preferred_element_type=jnp.float32)
            + lax.dot_general(lhs, low, contract, preferred_element_type=jnp.float32))

    def terms(row, piece):
        return pl.ds(pl.multiple_of(row * tall + piece * part, part), part)

    for step in range(1, half + 1):
        for piece in range(2):
            for way in range(2):
                if step == 1 and piece != way:
                    continue
                far = half - step + 1
                dest = behind[rc - far] if way == 0 else behind[far]
                if step == 1 or (step == 2 and piece != way):
                    src = gram.at[terms(dest, piece)]
                else:
                    src = rin.at[way, step - 2, piece]
                    arrived(src, rs_send.at[way, step - 2, piece],
                            rs_recv.at[way, step - 2, piece],
                            (left if way == 0 else right, c))
                    src[...] += gram[terms(dest, piece), :]
                send(src, rin.at[way, step - 1, piece], rs_send.at[way, step - 1, piece],
                     rs_recv.at[way, step - 1, piece], (right if way == 0 else left, c))
    for piece in range(2):
        for way in range(2):
            dst = rin.at[way, half - 1, piece]
            arrived(dst, rs_send.at[way, half - 1, piece], rs_recv.at[way, half - 1, piece],
                    (left if way == 0 else right, c))
        out[pl.ds(piece * part, part), :] = (
            gram[terms(r, piece), :] + rin[0, half - 1, piece] + rin[1, half - 1, piece])
    for copy in sent:
        copy.wait_send()


def shards(order, coeffs, h_blocks, block_codes):
    rc = lax.axis_size("row")
    cc = lax.axis_size("col")
    rows_here, orbitals = coeffs.shape
    tb = rows_here * cc // BLK
    nx = cc // 2
    half = rc // 2
    tall, width = orbitals // rc, orbitals // cc
    blocks = h_blocks.reshape(rc, CAP, BLK, BLK)
    codes = block_codes.reshape(rc, CAP)
    items = nx + 1 + rc
    dma = pltpu.SemaphoreType.DMA
    vmem = pl.BlockSpec(memory_space=pltpu.VMEM)
    peers = max(nx - 1, 1)
    return pl.pallas_call(
        functools.partial(kernel, order, rc, cc),
        out_shape=jax.ShapeDtypeStruct((tall, width), jnp.float32),
        in_specs=[vmem] * 3,
        out_specs=vmem,
        scratch_shapes=[
            pltpu.VMEM((cc, rows_here, orbitals), jnp.bfloat16),
            pltpu.VMEM((cc, rc, CAP, BLK, BLK), jnp.bfloat16),
            pltpu.VMEM((cc, rc, CAP), jnp.int32),
            pltpu.VMEM((rc, cc, rows_here, width), jnp.bfloat16),
            pltpu.VMEM((tb * BLK, width), jnp.float32),
            pltpu.VMEM((tb * BLK, 2 * BLK), jnp.bfloat16),
            pltpu.VMEM((orbitals, width), jnp.float32),
            pltpu.VMEM((2, half, 2, tall // 2, width), jnp.float32),
            dma((3,)),
            dma((peers, items)), dma((peers, items)),
            dma((peers, items)), dma((peers, items)),
            dma((3,)), dma((3,)),
            dma((2, half, cc)), dma((2, half, cc)),
            dma((2, half, 2)), dma((2, half, 2)),
        ],
        compiler_params=pltpu.CompilerParams(
            collective_id=0, has_side_effects=True, vmem_limit_bytes=63 * 1024 * 1024),
    )(coeffs, blocks, codes)


def solution(mesh):
    return jax.shard_map(
        functools.partial(shards, ring_order(mesh)),
        mesh=mesh,
        in_specs=(
            P(("row", "col"), None),
            P("row", "col", None, None, None, None),
            P("row", "col", None, None),
        ),
        out_specs=P("row", "col"),
        check_vma=False,
    )
```

```python
import functools

import jax
import jax.numpy as jnp
from jax import lax
from jax.experimental import pallas as pl
from jax.experimental.pallas import tpu as pltpu
from jax.sharding import PartitionSpec as P

BLK = 128
CAP = 4
RS_PIECES = 4
MESH = pl.DeviceIdType.MESH


def ring_order(mesh):
    rows = mesh.shape["row"]
    devices = mesh.devices.reshape(rows, -1)[:, 0]
    try:
        spots = [tuple(int(v) for v in d.coords) for d in devices]
    except (AttributeError, TypeError):
        return list(range(rows))
    axes = [a for a in range(len(spots[0])) if len({s[a] for s in spots}) > 1]
    if len(axes) != 2 or len(set(spots)) != rows:
        return list(range(rows))
    index = {(s[axes[0]], s[axes[1]]): i for i, s in enumerate(spots)}
    first = sorted({s[axes[0]] for s in spots})
    second = sorted({s[axes[1]] for s in spots})
    if len(first) % 2:
        return list(range(rows))
    cycle = []
    for n, a in enumerate(first):
        inner = second[1:] if n % 2 == 0 else second[:0:-1]
        cycle += [(a, b) for b in inner]
    cycle += [(a, second[0]) for a in reversed(first)]
    return [index[key] for key in cycle]


def kernel(order, rc, cc, coeffs, blocks, codes, out,
           cr, hall, codes_all, g, acc, dense, gram, rin,
           local_sem, dir_send, dir_recv, par_send, par_recv,
           own_send, own_recv, ring_send, ring_recv, rs_send, rs_recv):
    r = lax.axis_index("row")
    c = lax.axis_index("col")
    x, k = c // 2, c % 2
    nx = cc // 2
    partner = c + 1 - 2 * k
    half = rc // 2
    width = out.shape[1]
    tall = out.shape[0]
    pieces = rin.shape[2]
    part = tall // pieces
    tb = dense.shape[0] // BLK

    def look(table, i):
        value = jnp.int32(table[0])
        for n in range(1, len(table)):
            value = jnp.where(i == n, jnp.int32(table[n]), value)
        return value

    place = [0] * rc
    for n, row in enumerate(order):
        place[row] = n
    pos = look(place, r)
    behind = [r] + [look(order, lax.rem(pos + rc - s, rc)) for s in range(1, rc)]
    left, right = behind[1], behind[rc - 1]

    def xcol(d, kk):
        return lax.rem(x + nx - d, nx) * 2 + kk

    def cols(i, w):
        return pl.ds(pl.multiple_of(i * w, w), w)

    barrier = pltpu.get_barrier_semaphore()
    friends = [(left, c), (right, c), (r, partner)]
    friends += [(r, xcol(d, k)) for d in range(1, nx)]
    for friend in friends:
        pl.semaphore_signal(barrier, inc=1, device_id=friend, device_id_type=MESH)
    pl.semaphore_wait(barrier, len(friends))

    sent = []

    def send(src, dst, ssem, rsem, device):
        copy = pltpu.make_async_remote_copy(
            src_ref=src, dst_ref=dst, send_sem=ssem, recv_sem=rsem,
            device_id=device, device_id_type=MESH)
        copy.start()
        sent.append(copy)

    def arrived(dst, ssem, rsem, device):
        pltpu.make_async_remote_copy(
            src_ref=dst, dst_ref=dst, send_sem=ssem, recv_sem=rsem,
            device_id=device, device_id_type=MESH).wait_recv()

    def item_ref(source, base_x, n):
        if n < nx:
            return cr.at[source, :, cols(lax.rem(base_x + n, nx), 2 * width)]
        if n == nx:
            return codes_all.at[source]
        return hall.at[source, behind[n - nx - 1]]

    def item_src(base_x, n):
        if n < nx:
            return coeffs.at[:, cols(lax.rem(base_x + n, nx), 2 * width)]
        if n == nx:
            return codes
        return blocks.at[behind[n - nx - 1]]

    def send_item(d, n):
        tx = lax.rem(x + d, nx)
        send(item_src(tx, n), item_ref(c, tx, n), dir_send.at[d - 1, n],
             dir_recv.at[d - 1, n], (r, tx * 2 + k))

    def relay_item(d, n):
        src = item_ref(xcol(d, k), x, n)
        arrived(src, dir_send.at[d - 1, n], dir_recv.at[d - 1, n], (r, xcol(d, k)))
        send(src, src, par_send.at[d - 1, n], par_recv.at[d - 1, n], (r, partner))

    def take_item(d, n):
        dst = item_ref(xcol(d, 1 - k), x, n)
        arrived(dst, par_send.at[d - 1, n], par_recv.at[d - 1, n], (r, partner))

    def moves(step, j, way):
        if step < 1 or step > half:
            return False
        if step == half and rc % 2 == 0:
            return (j % 2) == way
        return True

    def slot(step, way):
        return step if way == 0 else rc - step

    def chunk_col(j):
        return xcol(j // 2, k if j % 2 == 0 else 1 - k)

    def ring_send_to(src, step, j, way):
        send(src, g.at[slot(step, way), chunk_col(j)], ring_send.at[way, step - 1, j],
             ring_recv.at[way, step - 1, j], (right if way == 0 else left, c))

    def ring_first(src, j):
        for way in range(2):
            if moves(1, j, way):
                ring_send_to(src, 1, j, way)

    copies = [
        pltpu.make_async_copy(coeffs, cr.at[c], local_sem.at[0]),
        pltpu.make_async_copy(blocks, hall.at[c], local_sem.at[1]),
        pltpu.make_async_copy(codes, codes_all.at[c], local_sem.at[2]),
    ]
    ring_first(coeffs.at[:, cols(c, width)], 0)
    for d in range(1, nx):
        send_item(d, 0)
    own = [(coeffs, cr.at[c], cr.at[partner]), (codes, codes_all.at[c], codes_all.at[partner]),
           (blocks, hall.at[c], hall.at[partner])]
    for n, (src, dst, _) in enumerate(own):
        send(src, dst, own_send.at[n], own_recv.at[n], (r, partner))
    for copy in copies:
        copy.start()
    hblock = nx + 1
    last_block = hblock + half
    for d in range(1, nx):
        send_item(d, nx)
    sequence = [0]
    for s in range(1, half):
        sequence += [s, rc - s]
    for s in sequence:
        for d in range(1, nx):
            send_item(d, hblock + s)
    for n in range(1, nx):
        for d in range(1, nx):
            send_item(d, n)
    for d in range(1, nx):
        send_item(d, last_block)

    def own_arrived(n):
        arrived(own[n][2], own_send.at[n], own_recv.at[n], (r, partner))

    own_arrived(0)
    ring_first(cr.at[partner, :, cols(c, width)], 1)
    for d in range(1, nx):
        relay_item(d, 0)
        ring_first(cr.at[xcol(d, k), :, cols(c, width)], 2 * d)
        take_item(d, 0)
        ring_first(cr.at[xcol(d, 1 - k), :, cols(c, width)], 2 * d + 1)
    for d in range(1, nx):
        relay_item(d, nx)
    for copy in copies:
        copy.wait()
    own_arrived(1)
    own_arrived(2)
    for d in range(1, nx):
        take_item(d, nx)

    acc[...] = jnp.zeros_like(acc)

    def accumulate(s, xx):
        p = behind[s]
        lane = lax.broadcasted_iota(jnp.int32, (CAP, rc), 1)
        for kk in range(2):
            tile = xx * 2 + kk
            marks = codes_all[tile]
            code = jnp.sum(jnp.where(lane == p, marks, 0), axis=1, keepdims=True)
            block = [hall[tile, p, t] for t in range(CAP)]
            for b in range(tb):
                hit = jnp.where(code == b, 1.0, 0.0).astype(jnp.float32)
                total = None
                for t in range(CAP):
                    pick = jnp.broadcast_to(hit[t:t + 1, :], (1, BLK)).astype(jnp.bfloat16)
                    term = block[t] * pick
                    total = term if total is None else total + term
                dense[pl.ds(b * BLK, BLK), pl.ds(kk * BLK, BLK)] = total
        if s == 0:
            rows = cr[pl.ds(xx * 2, 2), :, cols(c, width)]
        else:
            rows = g[s, pl.ds(xx * 2, 2)]
        acc[...] += jnp.dot(dense[...], rows.reshape(2 * BLK, width),
                            preferred_element_type=jnp.float32)

    def at_distance(s):
        if s == 0 or (2 * s == rc):
            return [s]
        return [s, rc - s]

    accumulate(0, x)
    for step in range(1, half + 1):
        for j in range(cc):
            for way in range(2):
                if moves(step, j, way):
                    here = g.at[slot(step, way), chunk_col(j)]
                    arrived(here, ring_send.at[way, step - 1, j],
                            ring_recv.at[way, step - 1, j],
                            (left if way == 0 else right, c))
                    if moves(step + 1, j, way):
                        ring_send_to(here, step + 1, j, way)
        for s in at_distance(step - 1):
            for d in range(1, nx):
                relay_item(d, hblock + s)
        for s in at_distance(step):
            accumulate(s, x)
        for s in at_distance(step - 1):
            for d in range(1, nx):
                take_item(d, hblock + s)
                accumulate(s, lax.rem(x + nx - d, nx))
    for n in range(1, nx):
        for d in range(1, nx):
            relay_item(d, n)
    for n in range(1, nx):
        for d in range(1, nx):
            take_item(d, n)
    for d in range(1, nx):
        relay_item(d, last_block)
    for d in range(1, nx):
        take_item(d, last_block)
        accumulate(half, lax.rem(x + nx - d, nx))

    applied = acc[...]
    high = applied.astype(jnp.bfloat16)
    low = (applied - high.astype(jnp.float32)).astype(jnp.bfloat16)
    contract = (((0,), (0,)), ((), ()))
    blockwise = tall % BLK == 0

    def gram_rows(start, size):
        lhs = cr[:, :, pl.ds(start, size)].reshape(cc * coeffs.shape[0], size)
        gram[pl.ds(start, size), :] = (
            lax.dot_general(lhs, high, contract, preferred_element_type=jnp.float32)
            + lax.dot_general(lhs, low, contract, preferred_element_type=jnp.float32))

    def gram_for(row):
        if blockwise:
            gram_rows(pl.multiple_of(row * tall, tall), tall)

    if not blockwise:
        for i in range(coeffs.shape[1] // BLK):
            gram_rows(i * BLK, BLK)

    def terms(row, piece):
        return pl.ds(pl.multiple_of(row * tall + piece * part, part), part)

    for step in range(1, half + 1):
        for s in at_distance(half - step + 1):
            gram_for(behind[s])
        for piece in range(pieces):
            for way in range(2):
                if step == 1 and piece % 2 != way:
                    continue
                far = half - step + 1
                dest = behind[rc - far] if way == 0 else behind[far]
                if step == 1 or (step == 2 and piece % 2 != way):
                    src = gram.at[terms(dest, piece)]
                else:
                    src = rin.at[way, step - 2, piece]
                    arrived(src, rs_send.at[way, step - 2, piece],
                            rs_recv.at[way, step - 2, piece],
                            (left if way == 0 else right, c))
                    src[...] += gram[terms(dest, piece), :]
                send(src, rin.at[way, step - 1, piece], rs_send.at[way, step - 1, piece],
                     rs_recv.at[way, step - 1, piece], (right if way == 0 else left, c))
    gram_for(r)
    for piece in range(pieces):
        for way in range(2):
            dst = rin.at[way, half - 1, piece]
            arrived(dst, rs_send.at[way, half - 1, piece], rs_recv.at[way, half - 1, piece],
                    (left if way == 0 else right, c))
        out[pl.ds(piece * part, part), :] = (
            gram[terms(r, piece), :] + rin[0, half - 1, piece] + rin[1, half - 1, piece])
    for copy in sent:
        copy.wait_send()


def shards(order, coeffs, h_blocks, block_codes):
    rc = lax.axis_size("row")
    cc = lax.axis_size("col")
    rows_here, orbitals = coeffs.shape
    tb = rows_here * cc // BLK
    nx = cc // 2
    half = rc // 2
    tall, width = orbitals // rc, orbitals // cc
    blocks = h_blocks.reshape(rc, CAP, BLK, BLK)
    codes = block_codes.reshape(rc, CAP).T
    items = nx + 1 + rc
    dma = pltpu.SemaphoreType.DMA
    vmem = pl.BlockSpec(memory_space=pltpu.VMEM)
    peers = max(nx - 1, 1)
    return pl.pallas_call(
        functools.partial(kernel, order, rc, cc),
        out_shape=jax.ShapeDtypeStruct((tall, width), jnp.float32),
        in_specs=[pl.BlockSpec(memory_space=pl.ANY)] * 3,
        out_specs=vmem,
        scratch_shapes=[
            pltpu.VMEM((cc, rows_here, orbitals), jnp.bfloat16),
            pltpu.VMEM((cc, rc, CAP, BLK, BLK), jnp.bfloat16),
            pltpu.VMEM((cc, CAP, rc), jnp.int32),
            pltpu.VMEM((rc, cc, rows_here, width), jnp.bfloat16),
            pltpu.VMEM((tb * BLK, width), jnp.float32),
            pltpu.VMEM((tb * BLK, 2 * BLK), jnp.bfloat16),
            pltpu.VMEM((orbitals, width), jnp.float32),
            pltpu.VMEM((2, half, RS_PIECES, tall // RS_PIECES, width), jnp.float32),
            dma((3,)),
            dma((peers, items)), dma((peers, items)),
            dma((peers, items)), dma((peers, items)),
            dma((3,)), dma((3,)),
            dma((2, half, cc)), dma((2, half, cc)),
            dma((2, half, RS_PIECES)), dma((2, half, RS_PIECES)),
        ],
        compiler_params=pltpu.CompilerParams(
            collective_id=0, has_side_effects=True, vmem_limit_bytes=63 * 1024 * 1024),
    )(coeffs, blocks, codes)


def solution(mesh):
    return jax.shard_map(
        functools.partial(shards, ring_order(mesh)),
        mesh=mesh,
        in_specs=(
            P(("row", "col"), None),
            P("row", "col", None, None, None, None),
            P("row", "col", None, None),
        ),
        out_specs=P("row", "col"),
        check_vma=False,
    )
```
